8 devices in a mesh: dp: 1 (over z), cpo: 2 (over y), cp: 4 (over x, core).
Axes of the slice: x: 2, y: 2, z: 1, core: 2. Of those that a mesh axis runs over, the one named last changes fastest.
Arguments:
- queries: bfloat16 [4, 8192, 4, 128], P('dp', ('cpo', 'cp'))
- key_seq: bfloat16 [4, 8192, 1, 128], P('dp', ('cpo', 'cp'))
- value_seq: bfloat16 [4, 8192, 1, 128], P('dp', ('cpo', 'cp'))
- out_grad: bfloat16 [4, 8192, 4, 128], P('dp', ('cpo', 'cp'))
Outputs:
- output 1: bfloat16 [4, 8192, 4, 128], P('dp', ('cpo', 'cp'))
- output 2: bfloat16 [4, 8192, 4, 128], P('dp', ('cpo', 'cp'))
- output 3: bfloat16 [4, 8192, 1, 128], P('dp', ('cpo', 'cp'))
- output 4: bfloat16 [4, 8192, 1, 128], P('dp', ('cpo', 'cp'))
All inputs are finite; a program needn't handle non-finite values.
Results may differ from the reference program's by a relative error of at most 0.00709.
Values are sent between devices in bfloat16 or wider.
A program may use at most 1 GiB of HBM per device.

```python
import math
import jax
import jax.numpy as jnp
from jax import lax

BATCH = 4
SEQ = 8192
SHARD_LEN = 1024
HEADS = 4
KV_HEADS = 1
HEAD = 128

GROUPS = HEADS // KV_HEADS
NBLK = SEQ // SHARD_LEN
SCORE_SCALE = HEAD ** -0.5


def setup_inputs(seed: int = 0, part: int = 0) -> dict:
    base_key = jax.random.fold_in(jax.random.key(seed), part)
    key_q, key_k, key_v, key_do = jax.random.split(base_key, 4)
    spread = math.sqrt(0.5 * math.log(SEQ))
    shape_q = (BATCH, SEQ, HEADS, HEAD)
    shape_kv = (BATCH, SEQ, KV_HEADS, HEAD)
    queries = spread * jax.random.normal(key_q, shape_q, jnp.float32)
    key_seq = jax.random.normal(key_k, shape_kv, jnp.float32)
    value_seq = jax.random.normal(key_v, shape_kv, jnp.float32)
    out_grad = jax.random.normal(key_do, shape_q, jnp.float32)
    return {'queries': queries.astype(jnp.bfloat16), 'key_seq': key_seq.astype(jnp.bfloat16), 'value_seq': value_seq.astype(jnp.bfloat16), 'out_grad': out_grad.astype(jnp.bfloat16)}


def query_rows(x_all, blk_idx):
    rows_blk = lax.dynamic_slice_in_dim(x_all, blk_idx * SHARD_LEN, SHARD_LEN, axis=1)
    return rows_blk.reshape(BATCH, SHARD_LEN, KV_HEADS, GROUPS, HEAD).astype(jnp.float32)


def kv_rows(x_all, blk_idx):
    return lax.dynamic_slice_in_dim(x_all, blk_idx * SHARD_LEN, SHARD_LEN, axis=1).astype(jnp.float32)


def to_bf16_values(x_val):
    return x_val.astype(jnp.bfloat16).astype(jnp.float32)


def block_scores(q_grp, k_blk, q_idx, k_idx):
    scores = jnp.einsum('bqhgd,bkhd->bhgqk', q_grp, k_blk) * SCORE_SCALE
    q_pos = q_idx * SHARD_LEN + jnp.arange(SHARD_LEN)
    k_pos = k_idx * SHARD_LEN + jnp.arange(SHARD_LEN)
    return jnp.where(q_pos[:, None] >= k_pos[None, :], scores, -jnp.inf)


def reference(queries, key_seq, value_seq, out_grad):
    stat_shape = (BATCH, KV_HEADS, GROUPS, SHARD_LEN)
    grp_shape = (BATCH, SHARD_LEN, KV_HEADS, GROUPS, HEAD)
    kv_shape = (BATCH, SHARD_LEN, KV_HEADS, HEAD)

    def forward_shard(q_idx):
        q_grp = query_rows(queries, q_idx)

        def key_step(k_idx, soft_state):
            acc_out, row_max, row_sum = soft_state
            scores = block_scores(q_grp, kv_rows(key_seq, k_idx), q_idx, k_idx)
            new_max = jnp.maximum(row_max, scores.max(axis=-1))
            rescale = jnp.exp(row_max - new_max)
            attn_prob = jnp.exp(scores - new_max[..., None])
            row_sum = row_sum * rescale + attn_prob.sum(axis=-1)
            pv_part = jnp.einsum('bhgqk,bkhd->bqhgd', to_bf16_values(attn_prob), kv_rows(value_seq, k_idx))
            acc_out = acc_out * jnp.transpose(rescale, (0, 3, 1, 2))[..., None] + pv_part
            return acc_out, new_max, row_sum

        start_state = (jnp.zeros(grp_shape, jnp.float32), jnp.full(stat_shape, -jnp.inf, jnp.float32), jnp.zeros(stat_shape, jnp.float32))
        acc_out, row_max, row_sum = lax.fori_loop(0, q_idx + 1, key_step, start_state)
        out_blk = (acc_out / jnp.transpose(row_sum, (0, 3, 1, 2))[..., None]).astype(jnp.bfloat16)
        return out_blk, row_max + jnp.log(row_sum)

    out_blks, log_sums = lax.map(forward_shard, jnp.arange(NBLK))
    attn_out = jnp.transpose(out_blks, (1, 0, 2, 3, 4, 5)).reshape(BATCH, SEQ, HEADS, HEAD)

    def grad_terms(q_idx, k_idx):
        q_grp = query_rows(queries, q_idx)
        do_grp = query_rows(out_grad, q_idx)
        o_grp = query_rows(attn_out, q_idx)
        k_blk = kv_rows(key_seq, k_idx)
        v_blk = kv_rows(value_seq, k_idx)
        row_dot = jnp.einsum('bqhgd,bqhgd->bhgq', do_grp, o_grp)
        attn_prob = jnp.exp(block_scores(q_grp, k_blk, q_idx, k_idx) - log_sums[q_idx][..., None])
        prob_grad = jnp.einsum('bqhgd,bkhd->bhgqk', do_grp, v_blk)
        score_grad = to_bf16_values(attn_prob * (prob_grad - row_dot[..., None]))
        return q_grp, do_grp, k_blk, attn_prob, score_grad

    def dq_shard(q_idx):
        def key_step(k_idx, dq_acc):
            q_grp, do_grp, k_blk, attn_prob, score_grad = grad_terms(q_idx, k_idx)
            return dq_acc + jnp.einsum('bhgqk,bkhd->bqhgd', score_grad, k_blk) * SCORE_SCALE

        dq_acc = lax.fori_loop(0, q_idx + 1, key_step, jnp.zeros(grp_shape, jnp.float32))
        return dq_acc.astype(jnp.bfloat16)

    def dkv_shard(k_idx):
        def query_step(q_idx, grad_pair):
            dk_acc, dv_acc = grad_pair
            q_grp, do_grp, k_blk, attn_prob, score_grad = grad_terms(q_idx, k_idx)
            dk_acc = dk_acc + jnp.einsum('bhgqk,bqhgd->bkhd', score_grad, q_grp) * SCORE_SCALE
            dv_acc = dv_acc + jnp.einsum('bhgqk,bqhgd->bkhd', to_bf16_values(attn_prob), do_grp)
            return dk_acc, dv_acc

        start_pair = (jnp.zeros(kv_shape, jnp.float32), jnp.zeros(kv_shape, jnp.float32))
        dk_acc, dv_acc = lax.fori_loop(k_idx, NBLK, query_step, start_pair)
        return dk_acc.astype(jnp.bfloat16), dv_acc.astype(jnp.bfloat16)

    dq_blks = lax.map(dq_shard, jnp.arange(NBLK))
    dk_blks, dv_blks = lax.map(dkv_shard, jnp.arange(NBLK))
    q_grad = jnp.transpose(dq_blks, (1, 0, 2, 3, 4, 5)).reshape(BATCH, SEQ, HEADS, HEAD)
    k_grad = jnp.transpose(dk_blks, (1, 0, 2, 3, 4)).reshape(BATCH, SEQ, KV_HEADS, HEAD)
    v_grad = jnp.transpose(dv_blks, (1, 0, 2, 3, 4)).reshape(BATCH, SEQ, KV_HEADS, HEAD)
    return (attn_out, q_grad, k_grad, v_grad)
```

```python
import functools
import math

import jax
import jax.numpy as jnp
from jax import lax
from jax.experimental import pallas as pl
from jax.experimental.pallas import tpu as pltpu
from jax.sharding import PartitionSpec as P

F32 = jnp.float32
BF16 = jnp.bfloat16
N_DEV = 8
N_SEQ = 4
SHARD = 1024
HEAD = 128
ROWS = 2 * SHARD
CHUNK = 1024
HALF = 512
SCALE = HEAD ** -0.5
LOG2_SCALE = SCALE * math.log2(math.e)
NT = (((1,), (1,)), ((), ()))
NN = (((1,), (0,)), ((), ()))
MESH_ID = pl.DeviceIdType.MESH


def dot(lhs, rhs, dims):
    return lax.dot_general(lhs, rhs, dims, preferred_element_type=F32)


def causal(scores, key_start, token_start, fill):
    key_pos = key_start + lax.broadcasted_iota(jnp.int32, scores.shape, 0)
    row_tok = token_start + lax.broadcasted_iota(jnp.int32, scores.shape, 1) // 2
    return jnp.where(key_pos <= row_tok, scores, fill)


def attn_kernel(q_in, k_in, v_in, do_in, o_out, dq_out, dkv_out,
                q_buf, k_buf, v_buf, do_buf, kt_buf, vt_buf, acc_t, dkv_acc, stage, part, dkv_stage, row_m, row_l,
                in_send, in_recv, out_send, out_recv, loc_sem):
    y_pos = lax.axis_index('cpo')
    b_pos = lax.axis_index('cp')
    x_pos = b_pos // 2
    core = b_pos % 2
    chip = y_pos * 2 + x_pos
    me = chip * 2 + core

    def dev(shard):
        return (lax.axis_index('dp'), shard // 4, shard % 4)

    def by_code(code):
        return ((y_pos + code // 4) % 2) * 4 + ((x_pos + (code // 2) % 2) % 2) * 2 + (core + code % 2) % 2

    def code_of(shard):
        return ((y_pos + shard // 4) % 2) * 4 + ((x_pos + (shard // 2) % 2) % 2) * 2 + (core + shard % 2) % 2

    def arrival(n):
        is3 = (n // 3) % 2 * (1 - n // 4)
        is4 = n // 4 - n // 5
        return n + is3 - is4

    def departure(n):
        u = n // 2
        mid = (u * (3 - u)) // 2
        rel = 3 * ((3 - u) // 3) + mid * (1 + n % 2)
        cidx = (1 - mid) * (n % 2) + mid * (u - 1)
        return ((y_pos + rel // 2) % 2) * 4 + ((x_pos + rel % 2) % 2) * 2 + cidx

    srcs = (k_in, v_in, q_in, do_in)
    bufs = (k_buf, v_buf, q_buf, do_buf)

    def in_copy(what, code):
        to = by_code(code)
        src = srcs[what].at[to // 2] if what < 2 else srcs[what].at[to // 2, to % 2]
        return pltpu.make_async_remote_copy(
            src_ref=src, dst_ref=bufs[what].at[me], send_sem=in_send.at[what, code], recv_sem=in_recv.at[what, code],
            device_id=dev(to), device_id_type=MESH_ID)

    def own_copy(what):
        src = srcs[what].at[chip] if what < 2 else srcs[what].at[chip, core]
        return pltpu.make_async_copy(src, bufs[what].at[me], loc_sem.at[what])

    barrier = pltpu.get_barrier_semaphore()
    for code in range(1, N_DEV):
        pl.semaphore_signal(barrier, inc=1, device_id=dev(by_code(code)), device_id_type=MESH_ID)
    for what in range(4):
        own_copy(what).start()
    pl.semaphore_wait(barrier, N_DEV - 1)

    for code in range(1, N_DEV):
        for what in range(3):
            in_copy(what, code).start()
    for code in range(1, N_DEV):
        in_copy(3, code).start()

    def fwd_scores(i, row0, j, nkeys):
        return dot(k_buf[j, pl.ds(0, nkeys), :], q_buf[i, pl.ds(row0, CHUNK), :], NT)

    def fwd_diag(i):
        for c in range(2):
            rows = pl.ds(c * CHUNK, CHUNK)
            nkeys = (c + 1) * HALF
            s_t = causal(fwd_scores(i, c * CHUNK, i, nkeys), 0, c * HALF, -jnp.inf)
            mx = jnp.max(s_t, axis=0, keepdims=True)
            p_t = jnp.exp2((s_t - mx) * LOG2_SCALE)
            row_m[i, :, rows] = mx
            row_l[i, :, rows] = jnp.sum(p_t, axis=0, keepdims=True)
            acc_t[i, :, rows] = dot(vt_buf[i, :, pl.ds(0, nkeys)], p_t.astype(BF16), NN)

    def fwd_full(i, j):
        s_all = [fwd_scores(i, c * CHUNK, j, SHARD) for c in range(2)]
        for c in range(2):
            rows = pl.ds(c * CHUNK, CHUNK)
            s_t = s_all[c]
            old = row_m[i, :, rows]
            mx = jnp.maximum(old, jnp.max(s_t, axis=0, keepdims=True))
            keep = jnp.exp2((old - mx) * LOG2_SCALE)
            p_t = jnp.exp2((s_t - mx) * LOG2_SCALE)
            row_m[i, :, rows] = mx
            row_l[i, :, rows] = row_l[i, :, rows] * keep + jnp.sum(p_t, axis=0, keepdims=True)
            acc_t[i, :, rows] = acc_t[i, :, rows] * keep + dot(vt_buf[j], p_t.astype(BF16), NN)

    def fwd_shard(n, first):
        code = arrival(n)
        new = by_code(code)
        if first:
            for what in range(3):
                own_copy(what).wait()
        else:
            for what in range(3):
                in_copy(what, code).wait_recv()
        kt_buf[new] = k_buf[new].T
        vt_buf[new] = v_buf[new].T
        fwd_diag(new)
        if not first:
            def pair(t, carry):
                old = by_code(arrival(t))
                fwd_full(jnp.maximum(new, old), jnp.minimum(new, old))
                return carry
            lax.fori_loop(0, n, pair, 0)

    fwd_shard(0, True)

    def fwd_loop(n, carry):
        fwd_shard(n, False)
        return carry
    lax.fori_loop(1, N_DEV, fwd_loop, 0)

    def out_copy(what, shard, code):
        src = dkv_stage.at[shard] if what == 2 else stage.at[shard]
        dst = dkv_out.at[core, chip] if what == 2 else (o_out, dq_out)[what].at[chip, core]
        return pltpu.make_async_remote_copy(
            src_ref=src, dst_ref=dst, send_sem=out_send.at[what, code], recv_sem=out_recv.at[what, code],
            device_id=dev(shard), device_id_type=MESH_ID)

    def out_own(what):
        src = dkv_stage.at[me] if what == 2 else stage.at[me]
        dst = dkv_out.at[core, chip] if what == 2 else (o_out, dq_out)[what].at[chip, core]
        return pltpu.make_async_copy(src, dst, loc_sem.at[4 + what])

    def start_out(what, shard):
        code = code_of(shard)

        @pl.when(code == 0)
        def _():
            out_own(what).start()

        @pl.when(code > 0)
        def _():
            out_copy(what, shard, code).start()

    def wait_out(what, shard):
        code = code_of(shard)

        @pl.when(code == 0)
        def _():
            out_own(what).wait()

        @pl.when(code > 0)
        def _():
            out_copy(what, shard, code).wait_send()

    own_copy(3).wait()

    def fin_loop(n, carry):
        shard = departure(n)
        code = code_of(shard)

        @pl.when(code > 0)
        def _():
            in_copy(3, code).wait_recv()

        for c in range(2):
            rows = pl.ds(c * CHUNK, CHUNK)
            total = row_l[shard, :, rows]
            o_t = (acc_t[shard, :, rows] * (1.0 / total)).astype(BF16)
            o_rows = o_t.T
            stage[shard, rows, :] = o_rows
            row_m[shard, :, rows] = row_m[shard, :, rows] * LOG2_SCALE + jnp.log2(total)
            prod = o_rows.astype(F32) * do_buf[shard, rows, :].astype(F32)
            row_l[shard, :, rows] = jnp.sum(prod.T, axis=0, keepdims=True)
            acc_t[shard, :, rows] = jnp.zeros((HEAD, CHUNK), F32)
        dkv_acc[0, shard] = jnp.zeros((SHARD, HEAD), F32)
        dkv_acc[1, shard] = jnp.zeros((SHARD, HEAD), F32)
        start_out(0, shard)
        return carry
    lax.fori_loop(0, N_DEV, fin_loop, 0)

    def bwd_block(i, row0, nrow, j, key0, nkeys, masked, token0):
        keys = pl.ds(key0, nkeys)
        k_blk = k_buf[j, keys, :]
        v_blk = v_buf[j, keys, :]
        s_all, dp_all = [], []
        starts = [row0 + c * HALF for c in range(nrow)]
        for r0 in starts:
            s_all.append(dot(k_blk, q_buf[i, pl.ds(r0, HALF), :], NT))
            dp_all.append(dot(v_blk, do_buf[i, pl.ds(r0, HALF), :], NT))
        p_all, ds_all = [], []
        for c, r0 in enumerate(starts):
            rows = pl.ds(r0, HALF)
            p_t = jnp.exp2(s_all[c] * LOG2_SCALE - row_m[i, :, rows])
            if masked:
                p_t = causal(p_t, key0, token0 + c * (HALF // 2), 0.0)
            p_all.append(p_t.astype(BF16))
            ds_all.append((p_t * (dp_all[c] - row_l[i, :, rows])).astype(BF16))
        dv_new, dk_new = None, None
        for c, r0 in enumerate(starts):
            rows = pl.ds(r0, HALF)
            dv_c = dot(p_all[c], do_buf[i, rows, :], NN)
            dk_c = dot(ds_all[c], q_buf[i, rows, :], NN)
            dv_new = dv_c if dv_new is None else dv_new + dv_c
            dk_new = dk_c if dk_new is None else dk_new + dk_c
        dkv_acc[0, j, keys, :] += dv_new
        dkv_acc[1, j, keys, :] += dk_new
        for c, r0 in enumerate(starts):
            rows = pl.ds(r0, HALF)
            acc_t[i, :, rows] += dot(kt_buf[j, :, keys], ds_all[c], NN)

    def bwd_diag(i):
        bwd_block(i, 0, 2, i, 0, HALF, True, 0)
        bwd_block(i, CHUNK, 2, i, 0, HALF, False, HALF)
        bwd_block(i, CHUNK, 2, i, HALF, HALF, True, HALF)

    def bwd_full(i, j):
        def chunk(c, carry):
            bwd_block(i, pl.multiple_of(c * CHUNK, CHUNK), 2, j, 0, SHARD, False, 0)
            return carry
        lax.fori_loop(0, 2, chunk, 0)

    def part_copy(shard):
        return pltpu.make_async_remote_copy(
            src_ref=dkv_acc.at[1 - core, shard], dst_ref=part.at[shard], send_sem=out_send.at[3, shard],
            recv_sem=out_recv.at[3, shard], device_id=dev(chip * 2 + 1 - core), device_id_type=MESH_ID)

    def finish_dkv(shard):
        part_copy(shard).wait_recv()
        factor = jnp.where(core == 0, 1.0, SCALE).astype(F32)
        dkv_stage[shard] = ((dkv_acc[core, shard] + part[shard]) * factor).astype(BF16)
        start_out(2, shard)

    def bwd_loop(n, carry):
        shard = departure(n)
        bwd_diag(shard)

        def pair(t, carry):
            other = departure(t)
            bwd_full(jnp.maximum(shard, other), jnp.minimum(shard, other))
            return carry
        lax.fori_loop(n + 1, N_DEV, pair, 0)
        part_copy(shard).start()
        wait_out(0, shard)
        for c in range(2):
            rows = pl.ds(c * CHUNK, CHUNK)
            stage[shard, rows, :] = (acc_t[shard, :, rows] * SCALE).astype(BF16).T
        start_out(1, shard)

        @pl.when(n > 0)
        def _():
            finish_dkv(departure(n - 1))
        return carry
    lax.fori_loop(0, N_DEV, bwd_loop, 0)
    finish_dkv(departure(N_DEV - 1))

    for code in range(1, N_DEV):
        for what in range(4):
            in_copy(what, code).wait_send()
    for n in range(N_DEV):
        shard = departure(n)
        part_copy(shard).wait_send()
        wait_out(1, shard)
        wait_out(2, shard)
    for code in range(1, N_DEV):
        for what in range(3):
            out_copy(what, by_code(code), code).wait_recv()


def local_attn(queries, key_seq, value_seq, out_grad):
    def split(x):
        x = x.reshape(N_SEQ, SHARD, 2, 2, HEAD)
        return jnp.transpose(x, (0, 2, 1, 3, 4)).reshape(N_SEQ, 2, ROWS, HEAD)

    def join(x):
        x = x.reshape(N_SEQ, 2, SHARD, 2, HEAD)
        return jnp.transpose(x, (0, 2, 1, 3, 4)).reshape(N_SEQ, SHARD, 4, HEAD)

    any_spec = pl.BlockSpec(memory_space=pl.ANY)
    o_x, dq_x, dkv_x = pl.pallas_call(
        attn_kernel,
        out_shape=(
            jax.ShapeDtypeStruct((N_SEQ, 2, ROWS, HEAD), BF16),
            jax.ShapeDtypeStruct((N_SEQ, 2, ROWS, HEAD), BF16),
            jax.ShapeDtypeStruct((2, N_SEQ, SHARD, HEAD), BF16),
        ),
        in_specs=[any_spec] * 4,
        out_specs=[any_spec] * 3,
        scratch_shapes=[
            pltpu.VMEM((N_DEV, ROWS, HEAD), BF16),
            pltpu.VMEM((N_DEV, SHARD, HEAD), BF16),
            pltpu.VMEM((N_DEV, SHARD, HEAD), BF16),
            pltpu.VMEM((N_DEV, ROWS, HEAD), BF16),
            pltpu.VMEM((N_DEV, HEAD, SHARD), BF16),
            pltpu.VMEM((N_DEV, HEAD, SHARD), BF16),
            pltpu.VMEM((N_DEV, HEAD, ROWS), F32),
            pltpu.VMEM((2, N_DEV, SHARD, HEAD), F32),
            pltpu.VMEM((N_DEV, ROWS, HEAD), BF16),
            pltpu.VMEM((N_DEV, SHARD, HEAD), F32),
            pltpu.VMEM((N_DEV, SHARD, HEAD), BF16),
            pltpu.VMEM((N_DEV, 1, ROWS), F32),
            pltpu.VMEM((N_DEV, 1, ROWS), F32),
            pltpu.SemaphoreType.DMA((4, N_DEV)),
            pltpu.SemaphoreType.DMA((4, N_DEV)),
            pltpu.SemaphoreType.DMA((4, N_DEV)),
            pltpu.SemaphoreType.DMA((4, N_DEV)),
            pltpu.SemaphoreType.DMA((7,)),
        ],
        compiler_params=pltpu.CompilerParams(
            collective_id=0, has_side_effects=True, vmem_limit_bytes=67043328),
        name='ctx_attn',
    )(split(queries), key_seq.reshape(N_SEQ, SHARD, HEAD), value_seq.reshape(N_SEQ, SHARD, HEAD), split(out_grad))
    k_grad = dkv_x[1].reshape(key_seq.shape)
    v_grad = dkv_x[0].reshape(value_seq.shape)
    return join(o_x), join(dq_x), k_grad, v_grad


def solution(mesh):
    seq_spec = P('dp', ('cpo', 'cp'), None, None)
    return jax.shard_map(local_attn, mesh=mesh, in_specs=(seq_spec,) * 4, out_specs=(seq_spec,) * 4, check_vma=False)
```

```python
import functools
import math

import jax
import jax.numpy as jnp
from jax import lax
from jax.experimental import pallas as pl
from jax.experimental.pallas import tpu as pltpu
from jax.sharding import PartitionSpec as P

F32 = jnp.float32
BF16 = jnp.bfloat16
N_DEV = 8
N_SEQ = 4
SHARD = 1024
HEAD = 128
ROWS = 2 * SHARD
SUB = 512
N_SUB = ROWS // SUB
SCALE = HEAD ** -0.5
LOG2_SCALE = SCALE * math.log2(math.e)
NN = (((1,), (0,)), ((), ()))
MESH_ID = pl.DeviceIdType.MESH


def dot(lhs, rhs, dims):
    return lax.dot_general(lhs, rhs, dims, preferred_element_type=F32)


def causal(scores, key_start, token_start, fill):
    key_pos = key_start + lax.broadcasted_iota(jnp.int32, scores.shape, 0)
    row_tok = token_start + lax.broadcasted_iota(jnp.int32, scores.shape, 1) // 2
    return jnp.where(key_pos <= row_tok, scores, fill)


def attn_kernel(q_in, k_in, v_in, do_in, o_out, dq_out, dkv_out,
                q_land, do_land, kv_buf, q_t, do_t, kv_t, acc_t, dkv_t, stage, part, p_rows, ds_rows, s_buf, row_m, row_l,
                in_send, in_recv, fwd_send, fwd_recv, out_send, out_recv, loc_sem):
    y_pos = lax.axis_index('cpo')
    b_pos = lax.axis_index('cp')
    x_pos = b_pos // 2
    core = b_pos % 2
    chip = y_pos * 2 + x_pos
    me = chip * 2 + core
    mate = chip * 2 + 1 - core

    def dev(shard):
        return (lax.axis_index('dp'), shard // 4, shard % 4)

    def chip_at(rel):
        return ((y_pos + rel // 2) % 2) * 2 + (x_pos + rel % 2) % 2

    def by_code(code):
        return chip_at(code // 2) * 2 + (core + code % 2) % 2

    def arrival(n):
        u = n // 2
        own = (3 - u) // 3
        rel = (u * (3 - u)) // 2 * (1 + n % 2) + 3 * (n // 6)
        late = n // 4 - n // 6
        cidx = n % 2 + late * (1 - 2 * (n % 2))
        return chip_at(rel) * 2 + own * ((core + n) % 2) + (1 - own) * cidx

    def departure(n):
        u = n // 2
        mid = (u * (3 - u)) // 2
        rel = 3 * ((3 - u) // 3) + mid * (1 + n % 2)
        cidx = (1 - mid) * (n % 2) + mid * (u - 1)
        return chip_at(rel) * 2 + cidx

    kv_in = (k_in, v_in)

    def kv_copy(what, to, source):
        return pltpu.make_async_remote_copy(
            src_ref=kv_in[what].at[to // 2], dst_ref=kv_buf.at[what, source],
            send_sem=in_send.at[what, to], recv_sem=in_recv.at[what, source], device_id=dev(to), device_id_type=MESH_ID)

    def kv_direct(source):
        return pltpu.make_async_remote_copy(
            src_ref=k_in.at[0], dst_ref=kv_buf.at[core, source],
            send_sem=in_send.at[core, source], recv_sem=in_recv.at[core, source], device_id=dev(mate), device_id_type=MESH_ID)

    def kv_pass(source, what):
        return pltpu.make_async_remote_copy(
            src_ref=kv_buf.at[what, source], dst_ref=kv_buf.at[what, source],
            send_sem=fwd_send.at[source], recv_sem=fwd_recv.at[source], device_id=dev(mate), device_id_type=MESH_ID)

    def row_copy(what, to, source):
        src, dst = (q_in, q_land) if what == 2 else (do_in, do_land)
        return pltpu.make_async_remote_copy(
            src_ref=src.at[to // 2, :, to % 2], dst_ref=dst.at[source],
            send_sem=in_send.at[what, to], recv_sem=in_recv.at[what, source], device_id=dev(to), device_id_type=MESH_ID)

    def own_copy(what):
        if what < 2:
            return pltpu.make_async_copy(kv_in[what].at[chip], kv_buf.at[what, me], loc_sem.at[what])
        src, dst = (q_in, q_land) if what == 2 else (do_in, do_land)
        return pltpu.make_async_copy(src.at[chip, :, core], dst.at[me], loc_sem.at[what])

    barrier = pltpu.get_barrier_semaphore()
    for code in range(1, N_DEV):
        pl.semaphore_signal(barrier, inc=1, device_id=dev(by_code(code)), device_id_type=MESH_ID)
    for what in range(4):
        own_copy(what).start()
    pl.semaphore_wait(barrier, N_DEV - 1)

    for what in range(2):
        kv_copy(what, mate, me).start()
    row_copy(2, mate, me).start()
    def send_kvq(rel):
        for what in range(2):
            kv_copy(what, chip_at(rel) * 2 + what, me).start()
        for cidx in range(2):
            row_copy(2, chip_at(rel) * 2 + cidx, me).start()

    def send_do():
        row_copy(3, mate, me).start()
        for rel in (3, 1, 2):
            for cidx in range(2):
                row_copy(3, chip_at(rel) * 2 + cidx, me).start()

    send_kvq(1 + core)

    def turn(land, dst, shard):
        for c in range(N_SUB):
            blk = land[shard, pl.ds(c * SUB // 2, SUB // 2)].reshape(SUB, HEAD)
            dst[shard, :, pl.ds(c * SUB, SUB)] = blk.T

    def fwd_diag(i):
        for c in range(N_SUB):
            rows = pl.ds(c * SUB, SUB)
            nkeys = (c + 1) * (SUB // 2)
            s_t = dot(kv_buf[0, i, pl.ds(0, nkeys), :], q_t[i, :, rows], NN)
            s_t = causal(s_t, 0, c * (SUB // 2), -jnp.inf)
            mx = jnp.max(s_t, axis=0, keepdims=True)
            p_t = jnp.exp2((s_t - mx) * LOG2_SCALE)
            row_m[i, :, rows] = mx
            row_l[i, :, rows] = jnp.sum(p_t, axis=0, keepdims=True)
            acc_t[i, :, rows] = dot(kv_t[i, :, pl.ds(0, nkeys)], p_t.astype(BF16), NN)

    def fwd_pairs(new, n):
        def place(step):
            old = arrival(step // N_SUB)
            return jnp.maximum(new, old), jnp.minimum(new, old), pl.ds(pl.multiple_of(step % N_SUB * SUB, SUB), SUB)

        def scores(step):
            i, j, rows = place(step)
            return dot(kv_buf[0, j], q_t[i, :, rows], NN)

        def softmax(step, slot):
            i, j, rows = place(step)
            s_t = s_buf[slot]
            old = row_m[i, :, rows]
            mx = jnp.maximum(old, jnp.max(s_t, axis=0, keepdims=True))
            keep = jnp.exp2((old - mx) * LOG2_SCALE)
            row_m[i, :, rows] = mx
            total, out = row_l[i, :, rows] * keep, acc_t[i, :, rows] * keep
            for k0 in range(0, SHARD, SHARD // 2):
                p_t = jnp.exp2((s_t[k0:k0 + SHARD // 2] - mx) * LOG2_SCALE)
                total += jnp.sum(p_t, axis=0, keepdims=True)
                out += dot(kv_t[j, :, pl.ds(k0, SHARD // 2)], p_t.astype(BF16), NN)
            row_l[i, :, rows] = total
            acc_t[i, :, rows] = out

        def two(step, carry):
            for slot in range(2):
                now = step * 2 + slot
                s_buf[1 - slot] = scores(jnp.minimum(now + 1, n * N_SUB - 1))
                softmax(now, slot)
            return carry

        @pl.when(n > 0)
        def _():
            s_buf[0] = scores(0)
            lax.fori_loop(0, n * (N_SUB // 2), two, 0)

    def fwd_loop(n, carry):
        new = arrival(n)

        @pl.when(n == 0)
        def _():
            for what in range(3):
                own_copy(what).wait()

        @pl.when(n == 1)
        def _():
            for what in range(2):
                kv_copy(what, mate, new).wait_recv()

        @pl.when(n > 0)
        def _():
            row_copy(2, mate, new).wait_recv()

        turn(q_land, q_t, new)

        @pl.when(n > 1)
        def _():
            kv_pass(new, 1 - core).wait_recv()

        kv_t[new] = kv_buf[1, new].T
        fwd_diag(new)

        fwd_pairs(new, n)

        @pl.when((n > 0) & (n < N_DEV - 1))
        def _():
            following = (arrival(n + 1))
            kv_direct(following).wait_recv()
            kv_pass(following, core).start()

        @pl.when(n == 1)
        def _():
            send_kvq(2 - core)

        @pl.when(n == 3 + core)
        def _():
            send_kvq(3)

        @pl.when(n == 5 - core)
        def _():
            send_do()
        return carry
    lax.fori_loop(0, N_DEV, fwd_loop, 0)
    for n in range(2, N_DEV):
        kv_pass(arrival(n), core).wait_send()

    def out_refs(what, shard):
        if what == 2:
            return kv_buf.at[0, shard], dkv_out.at[core, chip]
        return stage.at[shard], (o_out, dq_out)[what].at[chip, core]

    def out_copy(what, shard, source):
        src, dst = out_refs(what, shard)
        return pltpu.make_async_remote_copy(
            src_ref=src, dst_ref=dst, send_sem=out_send.at[what, shard], recv_sem=out_recv.at[what, source],
            device_id=dev(shard), device_id_type=MESH_ID)

    def out_own(what):
        src, dst = out_refs(what, me)
        return pltpu.make_async_copy(src, dst, loc_sem.at[4 + what])

    def start_out(what, shard):
        @pl.when(shard == me)
        def _():
            out_own(what).start()

        @pl.when(shard != me)
        def _():
            out_copy(what, shard, me).start()

    def wait_out(what, shard):
        @pl.when(shard == me)
        def _():
            out_own(what).wait()

        @pl.when(shard != me)
        def _():
            out_copy(what, shard, me).wait_send()

    def finish_fwd(shard):
        @pl.when(shard == me)
        def _():
            own_copy(3).wait()

        @pl.when(shard != me)
        def _():
            row_copy(3, mate, shard).wait_recv()

        turn(do_land, do_t, shard)
        kv_t[shard] = kv_buf[0, shard].T
        for c in range(N_SUB):
            rows = pl.ds(c * SUB, SUB)
            total = row_l[shard, :, rows]
            o_c = (acc_t[shard, :, rows] * (1.0 / total)).astype(BF16)
            stage[shard, rows, :] = o_c.T
            row_m[shard, :, rows] = row_m[shard, :, rows] * LOG2_SCALE + jnp.log2(total)
            row_l[shard, :, rows] = jnp.sum(o_c.astype(F32) * do_t[shard, :, rows].astype(F32), axis=0, keepdims=True)
            acc_t[shard, :, rows] = jnp.zeros((HEAD, SUB), F32)
        dkv_t[0, shard] = jnp.zeros((HEAD, SHARD), F32)
        dkv_t[1, shard] = jnp.zeros((HEAD, SHARD), F32)
        start_out(0, shard)

    def bwd_block(i, row0, j, nkeys, token0, slot):
        keys = pl.ds(0, nkeys)
        rows = pl.ds(row0, SUB)
        s_t = dot(kv_buf[0, j, keys, :], q_t[i, :, rows], NN)
        dp_t = dot(kv_buf[1, j, keys, :], do_t[i, :, rows], NN)
        p_t = jnp.exp2(s_t * LOG2_SCALE - row_m[i, :, rows])
        if token0 is not None:
            p_t = causal(p_t, 0, token0, 0.0)
        ds_t = (p_t * (dp_t - row_l[i, :, rows])).astype(BF16)
        p_rows[slot, :, keys] = p_t.astype(BF16).T
        ds_rows[slot, :, keys] = ds_t.T
        acc_t[i, :, rows] += dot(kv_t[j, :, keys], ds_t, NN)
        dkv_t[0, j, :, keys] += dot(do_t[i, :, rows], p_rows[slot, :, keys], NN)
        dkv_t[1, j, :, keys] += dot(q_t[i, :, rows], ds_rows[slot, :, keys], NN)

    def bwd_diag(i):
        for c in range(N_SUB):
            bwd_block(i, c * SUB, i, (c + 1) * (SUB // 2), c * (SUB // 2), c % 2)

    def bwd_full(i, j):
        def two(c, carry):
            for slot in range(2):
                bwd_block(i, pl.multiple_of(c * (2 * SUB) + slot * SUB, SUB), j, SHARD, None, slot)
            return carry
        lax.fori_loop(0, N_SUB // 2, two, 0)

    def part_copy(shard):
        return pltpu.make_async_remote_copy(
            src_ref=dkv_t.at[1 - core, shard], dst_ref=part.at[shard], send_sem=out_send.at[3, shard],
            recv_sem=out_recv.at[3, shard], device_id=dev(mate), device_id_type=MESH_ID)

    def finish_dkv(shard):
        part_copy(shard).wait_recv()
        factor = jnp.where(core == 0, 1.0, SCALE).astype(F32)
        kv_buf[0, shard] = ((dkv_t[core, shard] + part[shard]) * factor).astype(BF16).T
        start_out(2, shard)

    finish_fwd(departure(0))

    def bwd_loop(n, carry):
        shard = departure(n)
        bwd_diag(shard)

        def pair(t, carry):
            other = departure(t)

            @pl.when(n == 0)
            def _():
                finish_fwd(other)

            bwd_full(jnp.maximum(shard, other), jnp.minimum(shard, other))
            return carry
        lax.fori_loop(n + 1, N_DEV, pair, 0)
        part_copy(shard).start()
        wait_out(0, shard)
        for c in range(N_SUB):
            rows = pl.ds(c * SUB, SUB)
            stage[shard, rows, :] = (acc_t[shard, :, rows] * SCALE).astype(BF16).T
        start_out(1, shard)

        @pl.when(n > 0)
        def _():
            finish_dkv(departure(n - 1))
        return carry
    lax.fori_loop(0, N_DEV, bwd_loop, 0)
    finish_dkv(departure(N_DEV - 1))

    for what in range(2):
        kv_copy(what, mate, me).wait_send()
        for rel in (1, 2, 3):
            kv_copy(what, chip_at(rel) * 2 + what, me).wait_send()
    for code in range(1, N_DEV):
        for what in (2, 3):
            row_copy(what, by_code(code), me).wait_send()
    for n in range(N_DEV):
        shard = departure(n)
        part_copy(shard).wait_send()
        wait_out(1, shard)
        wait_out(2, shard)
    for code in range(1, N_DEV):
        source = by_code(code)
        for what in range(3):
            out_copy(what, source, source).wait_recv()


def local_attn(queries, key_seq, value_seq, out_grad):
    def join(x):
        x = x.reshape(N_SEQ, 2, SHARD, 2, HEAD)
        return jnp.transpose(x, (0, 2, 1, 3, 4)).reshape(N_SEQ, SHARD, 4, HEAD)

    any_spec = pl.BlockSpec(memory_space=pl.ANY)
    o_x, dq_x, dkv_x = pl.pallas_call(
        attn_kernel,
        out_shape=(
            jax.ShapeDtypeStruct((N_SEQ, 2, ROWS, HEAD), BF16),
            jax.ShapeDtypeStruct((N_SEQ, 2, ROWS, HEAD), BF16),
            jax.ShapeDtypeStruct((2, N_SEQ, SHARD, HEAD), BF16),
        ),
        in_specs=[any_spec] * 4,
        out_specs=[any_spec] * 3,
        scratch_shapes=[
            pltpu.VMEM((N_DEV, SHARD, 2, HEAD), BF16),
            pltpu.VMEM((N_DEV, SHARD, 2, HEAD), BF16),
            pltpu.VMEM((2, N_DEV, SHARD, HEAD), BF16),
            pltpu.VMEM((N_DEV, HEAD, ROWS), BF16),
            pltpu.VMEM((N_DEV, HEAD, ROWS), BF16),
            pltpu.VMEM((N_DEV, HEAD, SHARD), BF16),
            pltpu.VMEM((N_DEV, HEAD, ROWS), F32),
            pltpu.VMEM((2, N_DEV, HEAD, SHARD), F32),
            pltpu.VMEM((N_DEV, ROWS, HEAD), BF16),
            pltpu.VMEM((N_DEV, HEAD, SHARD), F32),
            pltpu.VMEM((2, SUB, SHARD), BF16),
            pltpu.VMEM((2, SUB, SHARD), BF16),
            pltpu.VMEM((2, SHARD, SUB), F32),
            pltpu.VMEM((N_DEV, 1, ROWS), F32),
            pltpu.VMEM((N_DEV, 1, ROWS), F32),
            pltpu.SemaphoreType.DMA((4, N_DEV)),
            pltpu.SemaphoreType.DMA((4, N_DEV)),
            pltpu.SemaphoreType.DMA((N_DEV,)),
            pltpu.SemaphoreType.DMA((N_DEV,)),
            pltpu.SemaphoreType.DMA((4, N_DEV)),
            pltpu.SemaphoreType.DMA((4, N_DEV)),
            pltpu.SemaphoreType.DMA((7,)),
        ],
        compiler_params=pltpu.CompilerParams(
            collective_id=0, has_side_effects=True, vmem_limit_bytes=67043328),
        name='ctx_attn',
    )(queries.reshape(N_SEQ, SHARD, 2, 2, HEAD), key_seq.reshape(N_SEQ, SHARD, HEAD),
      value_seq.reshape(N_SEQ, SHARD, HEAD), out_grad.reshape(N_SEQ, SHARD, 2, 2, HEAD))
    k_grad = dkv_x[1].reshape(key_seq.shape)
    v_grad = dkv_x[0].reshape(value_seq.shape)
    return join(o_x), join(dq_x), k_grad, v_grad


def solution(mesh):
    seq_spec = P('dp', ('cpo', 'cp'), None, None)
    return jax.shard_map(local_attn, mesh=mesh, in_specs=(seq_spec,) * 4, out_specs=(seq_spec,) * 4, check_vma=False)
```

```python
import functools
import math

import jax
import jax.numpy as jnp
from jax import lax
from jax.experimental import pallas as pl
from jax.experimental.pallas import tpu as pltpu
from jax.sharding import PartitionSpec as P

F32 = jnp.float32
BF16 = jnp.bfloat16
N_DEV = 8
N_SEQ = 4
SHARD = 1024
HEAD = 128
ROWS = 2 * SHARD
SUB = 512
N_SUB = ROWS // SUB
SCALE = HEAD ** -0.5
LOG2_SCALE = SCALE * math.log2(math.e)
NN = (((1,), (0,)), ((), ()))
MESH_ID = pl.DeviceIdType.MESH


def dot(lhs, rhs, dims):
    return lax.dot_general(lhs, rhs, dims, preferred_element_type=F32)


def causal(scores, key_start, token_start, fill):
    key_pos = key_start + lax.broadcasted_iota(jnp.int32, scores.shape, 0)
    row_tok = token_start + lax.broadcasted_iota(jnp.int32, scores.shape, 1) // 2
    return jnp.where(key_pos <= row_tok, scores, fill)


def attn_kernel(q_in, k_in, v_in, do_in, o_out, dq_out, dkv_out,
                q_land, do_land, kv_buf, q_t, do_t, kv_t, acc_t, dkv_t, stage, part, p_rows, ds_rows, s_buf, row_m, row_l,
                in_send, in_recv, fwd_send, fwd_recv, out_send, out_recv, loc_sem):
    y_pos = lax.axis_index('cpo')
    b_pos = lax.axis_index('cp')
    x_pos = b_pos // 2
    core = b_pos % 2
    chip = y_pos * 2 + x_pos
    me = chip * 2 + core
    mate = chip * 2 + 1 - core

    def dev(shard):
        return (lax.axis_index('dp'), shard // 4, shard % 4)

    def chip_at(rel):
        return ((y_pos + rel // 2) % 2) * 2 + (x_pos + rel % 2) % 2

    def by_code(code):
        return chip_at(code // 2) * 2 + (core + code % 2) % 2

    def arrival(n):
        u = n // 2
        near = (u * (3 - u)) // 2
        late = n // 4 - n // 6
        far = n // 6
        bit = (core + n % 2) % 2
        rel = near * ((1 - late) * (1 + bit) + late * (2 - bit)) + 3 * far
        return chip_at(rel) * 2 + (1 - far) * bit + far * (n % 2)

    def departure(n):
        u = n // 2
        mid = (u * (3 - u)) // 2
        rel = 3 * ((3 - u) // 3) + mid * (1 + n % 2)
        cidx = (1 - mid) * (n % 2) + mid * (u - 1)
        return chip_at(rel) * 2 + cidx

    kv_in = (k_in, v_in)

    def kv_copy(what, to, source):
        return pltpu.make_async_remote_copy(
            src_ref=kv_in[what].at[to // 2], dst_ref=kv_buf.at[what, source],
            send_sem=in_send.at[what, to], recv_sem=in_recv.at[what, source], device_id=dev(to), device_id_type=MESH_ID)

    def kv_direct(source):
        return pltpu.make_async_remote_copy(
            src_ref=k_in.at[0], dst_ref=kv_buf.at[core, source],
            send_sem=in_send.at[core, source], recv_sem=in_recv.at[core, source], device_id=dev(mate), device_id_type=MESH_ID)

    def kv_pass(source, what):
        return pltpu.make_async_remote_copy(
            src_ref=kv_buf.at[what, source], dst_ref=kv_buf.at[what, source],
            send_sem=fwd_send.at[source], recv_sem=fwd_recv.at[source], device_id=dev(mate), device_id_type=MESH_ID)

    def row_copy(what, to, source):
        src, dst = (q_in, q_land) if what == 2 else (do_in, do_land)
        return pltpu.make_async_remote_copy(
            src_ref=src.at[to // 2, :, to % 2], dst_ref=dst.at[source],
            send_sem=in_send.at[what, to], recv_sem=in_recv.at[what, source], device_id=dev(to), device_id_type=MESH_ID)

    def own_copy(what):
        if what < 2:
            return pltpu.make_async_copy(kv_in[what].at[chip], kv_buf.at[what, me], loc_sem.at[what])
        src, dst = (q_in, q_land) if what == 2 else (do_in, do_land)
        return pltpu.make_async_copy(src.at[chip, :, core], dst.at[me], loc_sem.at[what])

    barrier = pltpu.get_barrier_semaphore()
    for code in range(1, N_DEV):
        pl.semaphore_signal(barrier, inc=1, device_id=dev(by_code(code)), device_id_type=MESH_ID)
    for what in range(4):
        own_copy(what).start()
    pl.semaphore_wait(barrier, N_DEV - 1)

    for what in range(2):
        kv_copy(what, mate, me).start()
    row_copy(2, mate, me).start()
    def send_kv(rel):
        for what in range(2):
            kv_copy(what, chip_at(rel) * 2 + what, me).start()

    def send_q(rel):
        for flip in range(2):
            row_copy(2, chip_at(rel) * 2 + (core + flip) % 2, me).start()

    def send_kvq(rel):
        send_kv(rel)
        send_q(rel)

    def send_do():
        row_copy(3, mate, me).start()
        for rel in (3, 1 + core):
            for flip in range(2):
                row_copy(3, chip_at(rel) * 2 + (core + flip) % 2, me).start()
        row_copy(3, chip_at(2 - core) * 2 + 1 - core, me).start()

    send_kv(1 + core)

    def turn(land, dst, shard):
        for c in range(N_SUB):
            blk = land[shard, pl.ds(c * SUB // 2, SUB // 2)].reshape(SUB, HEAD)
            dst[shard, :, pl.ds(c * SUB, SUB)] = blk.T

    def fwd_diag(i):
        part_keys = SUB // 2

        def scores(c):
            rows = pl.ds(c * SUB, SUB)
            last = dot(kv_buf[0, i, pl.ds(c * part_keys, part_keys), :], q_t[i, :, rows], NN)
            if c == 0:
                return None, last
            return dot(kv_buf[0, i, pl.ds(0, c * part_keys), :], q_t[i, :, rows], NN), last

        here = scores(0)
        for c in range(N_SUB):
            following = scores(c + 1) if c + 1 < N_SUB else None
            rows = pl.ds(c * SUB, SUB)
            first, last = here
            last = causal(last, 0, 0, -jnp.inf)
            mx = jnp.max(last, axis=0, keepdims=True)
            if first is not None:
                mx = jnp.maximum(mx, jnp.max(first, axis=0, keepdims=True))
            p_t = jnp.exp2((last - mx) * LOG2_SCALE)
            total = jnp.sum(p_t, axis=0, keepdims=True)
            out = dot(kv_t[i, :, pl.ds(c * part_keys, part_keys)], p_t.astype(BF16), NN)
            if first is not None:
                p_t = jnp.exp2((first - mx) * LOG2_SCALE)
                total += jnp.sum(p_t, axis=0, keepdims=True)
                out += dot(kv_t[i, :, pl.ds(0, c * part_keys)], p_t.astype(BF16), NN)
            row_m[i, :, rows] = mx
            row_l[i, :, rows] = total
            acc_t[i, :, rows] = out
            here = following

    def pass_on(shard):
        kv_direct(shard).wait_recv()
        kv_pass(shard, core).start()

    def beside_last(n):
        @pl.when(n == 2)
        def _():
            send_kv(2 - core)
            row_copy(3, chip_at(2 - core) * 2 + core, me).start()

        @pl.when(n == 3)
        def _():
            pass_on(arrival(4))
            pass_on(arrival(5))
            send_q(2 - core)

    def fwd_pairs(new, n):
        def place(step):
            old = arrival(step // N_SUB)
            return jnp.maximum(new, old), jnp.minimum(new, old), pl.ds(pl.multiple_of(step % N_SUB * SUB, SUB), SUB)

        def scores(step):
            i, j, rows = place(step)
            return dot(kv_buf[0, j], q_t[i, :, rows], NN)

        def softmax(step, slot):
            i, j, rows = place(step)
            s_t = s_buf[slot]
            old = row_m[i, :, rows]
            mx = jnp.maximum(old, jnp.max(s_t, axis=0, keepdims=True))
            keep = jnp.exp2((old - mx) * LOG2_SCALE)
            row_m[i, :, rows] = mx
            total, out = row_l[i, :, rows] * keep, acc_t[i, :, rows] * keep
            for k0 in range(0, SHARD, SHARD // 2):
                p_t = jnp.exp2((s_t[k0:k0 + SHARD // 2] - mx) * LOG2_SCALE)
                total += jnp.sum(p_t, axis=0, keepdims=True)
                out += dot(kv_t[j, :, pl.ds(k0, SHARD // 2)], p_t.astype(BF16), NN)
            row_l[i, :, rows] = total
            acc_t[i, :, rows] = out

        def two(step, carry):
            @pl.when(step == (n - 1) * (N_SUB // 2))
            def _():
                beside_last(n)

            for slot in range(2):
                now = step * 2 + slot
                s_buf[1 - slot] = scores(jnp.minimum(now + 1, n * N_SUB - 1))
                softmax(now, slot)
            return carry

        @pl.when(n > 0)
        def _():
            s_buf[0] = scores(0)
            lax.fori_loop(0, n * (N_SUB // 2), two, 0)

    def fwd_loop(n, carry):
        new = arrival(n)

        @pl.when(n == 0)
        def _():
            for what in range(3):
                own_copy(what).wait()

        @pl.when(n == 1)
        def _():
            for what in range(2):
                kv_copy(what, mate, new).wait_recv()

        @pl.when(n > 0)
        def _():
            row_copy(2, mate, new).wait_recv()

        turn(q_land, q_t, new)

        @pl.when(n > 1)
        def _():
            kv_pass(new, 1 - core).wait_recv()

        kv_t[new] = kv_buf[1, new].T
        fwd_diag(new)

        @pl.when(n == 4 + 4 * core)
        def _():
            send_kvq(3)

        @pl.when(n == 5)
        def _():
            pass_on(arrival(6))

            @pl.when(core == 1)
            def _():
                send_kvq(3)

        @pl.when(n == 6)
        def _():
            pass_on(arrival(7))
            send_do()

        fwd_pairs(new, n)

        @pl.when(n == 0)
        def _():
            pass_on(arrival(2))
            pass_on(arrival(3))
            send_q(1 + core)

        return carry
    lax.fori_loop(0, N_DEV, fwd_loop, 0)
    for n in range(2, N_DEV):
        kv_pass(arrival(n), core).wait_send()

    def out_refs(what, shard):
        if what == 2:
            return kv_buf.at[0, shard], dkv_out.at[core, chip]
        return stage.at[shard], (o_out, dq_out)[what].at[chip, core]

    def out_copy(what, shard, source):
        src, dst = out_refs(what, shard)
        return pltpu.make_async_remote_copy(
            src_ref=src, dst_ref=dst, send_sem=out_send.at[what, shard], recv_sem=out_recv.at[what, source],
            device_id=dev(shard), device_id_type=MESH_ID)

    def out_own(what):
        src, dst = out_refs(what, me)
        return pltpu.make_async_copy(src, dst, loc_sem.at[4 + what])

    def start_out(what, shard):
        @pl.when(shard == me)
        def _():
            out_own(what).start()

        @pl.when(shard != me)
        def _():
            out_copy(what, shard, me).start()

    def wait_out(what, shard):
        @pl.when(shard == me)
        def _():
            out_own(what).wait()

        @pl.when(shard != me)
        def _():
            out_copy(what, shard, me).wait_send()

    def finish_fwd(shard):
        @pl.when(shard == me)
        def _():
            own_copy(3).wait()

        @pl.when(shard != me)
        def _():
            row_copy(3, mate, shard).wait_recv()

        turn(do_land, do_t, shard)
        kv_t[shard] = kv_buf[0, shard].T
        for c in range(N_SUB):
            rows = pl.ds(c * SUB, SUB)
            total = row_l[shard, :, rows]
            o_c = (acc_t[shard, :, rows] * (1.0 / total)).astype(BF16)
            stage[shard, rows, :] = o_c.T
            row_m[shard, :, rows] = row_m[shard, :, rows] * LOG2_SCALE + jnp.log2(total)
            row_l[shard, :, rows] = jnp.sum(o_c.astype(F32) * do_t[shard, :, rows].astype(F32), axis=0, keepdims=True)
            acc_t[shard, :, rows] = jnp.zeros((HEAD, SUB), F32)
        dkv_t[0, shard] = jnp.zeros((HEAD, SHARD), F32)
        dkv_t[1, shard] = jnp.zeros((HEAD, SHARD), F32)
        start_out(0, shard)

    def bwd_block(i, row0, j, nkeys, token0, slot):
        keys = pl.ds(0, nkeys)
        rows = pl.ds(row0, SUB)
        s_t = dot(kv_buf[0, j, keys, :], q_t[i, :, rows], NN)
        dp_t = dot(kv_buf[1, j, keys, :], do_t[i, :, rows], NN)
        p_t = jnp.exp2(s_t * LOG2_SCALE - row_m[i, :, rows])
        if token0 is not None:
            p_t = causal(p_t, 0, token0, 0.0)
        ds_t = (p_t * (dp_t - row_l[i, :, rows])).astype(BF16)
        p_rows[slot, :, keys] = p_t.astype(BF16).T
        ds_rows[slot, :, keys] = ds_t.T
        acc_t[i, :, rows] += dot(kv_t[j, :, keys], ds_t, NN)
        dkv_t[0, j, :, keys] += dot(do_t[i, :, rows], p_rows[slot, :, keys], NN)
        dkv_t[1, j, :, keys] += dot(q_t[i, :, rows], ds_rows[slot, :, keys], NN)

    def bwd_diag(i):
        for c in range(N_SUB):
            bwd_block(i, c * SUB, i, (c + 1) * (SUB // 2), c * (SUB // 2), c % 2)

    def bwd_full(i, j):
        def two(c, carry):
            for slot in range(2):
                bwd_block(i, pl.multiple_of(c * (2 * SUB) + slot * SUB, SUB), j, SHARD, None, slot)
            return carry
        lax.fori_loop(0, N_SUB // 2, two, 0)

    def part_copy(shard):
        return pltpu.make_async_remote_copy(
            src_ref=dkv_t.at[1 - core, shard], dst_ref=part.at[shard], send_sem=out_send.at[3, shard],
            recv_sem=out_recv.at[3, shard], device_id=dev(mate), device_id_type=MESH_ID)

    def finish_dkv(shard):
        part_copy(shard).wait_recv()
        factor = jnp.where(core == 0, 1.0, SCALE).astype(F32)
        kv_buf[0, shard] = ((dkv_t[core, shard] + part[shard]) * factor).astype(BF16).T
        start_out(2, shard)

    finish_fwd(departure(0))

    def bwd_loop(n, carry):
        shard = departure(n)
        bwd_diag(shard)

        @pl.when(n > 4)
        def _():
            finish_dkv(departure(n - 1))

        def pair(back, carry):
            t = N_DEV + n - back
            u = t // 2
            first = 1 - (n + 7) // 8
            other = departure(t + first * core * ((u * (3 - u)) // 2) * (1 - 2 * (t % 2)))

            @pl.when(n == 0)
            def _():
                finish_fwd(other)

            bwd_full(jnp.maximum(shard, other), jnp.minimum(shard, other))
            return carry
        lax.fori_loop(n + 1, N_DEV, pair, 0)
        part_copy(shard).start()
        wait_out(0, shard)
        for c in range(N_SUB):
            rows = pl.ds(c * SUB, SUB)
            stage[shard, rows, :] = (acc_t[shard, :, rows] * SCALE).astype(BF16).T
        start_out(1, shard)

        @pl.when((n > 0) & (n < 5))
        def _():
            finish_dkv(departure(n - 1))
        return carry
    lax.fori_loop(0, N_DEV, bwd_loop, 0)
    finish_dkv(departure(N_DEV - 1))

    for what in range(2):
        kv_copy(what, mate, me).wait_send()
        for rel in (1, 2, 3):
            kv_copy(what, chip_at(rel) * 2 + what, me).wait_send()
    for code in range(1, N_DEV):
        for what in (2, 3):
            row_copy(what, by_code(code), me).wait_send()
    for n in range(N_DEV):
        shard = departure(n)
        part_copy(shard).wait_send()
        wait_out(1, shard)
        wait_out(2, shard)
    for code in range(1, N_DEV):
        source = by_code(code)
        for what in range(3):
            out_copy(what, source, source).wait_recv()


def join_kernel(o_in, dq_in, dkv_in, o_out, dq_out, dk_out, dv_out, rows, keys, get_sem, put_sem):
    moves = []
    for which, (src, dst) in enumerate(((o_in, o_out), (dq_in, dq_out))):
        for seq in range(N_SEQ):
            for pair in range(2):
                moves.append((src.at[seq, pair], rows.at[which, seq, pair], dst.at[seq, :, pair]))
    for which, dst in enumerate((dv_out, dk_out)):
        moves.append((dkv_in.at[which], keys.at[which], dst))
    gets = [pltpu.make_async_copy(src, mid, get_sem.at[n]) for n, (src, mid, dst) in enumerate(moves)]
    puts = [pltpu.make_async_copy(mid, dst, put_sem.at[n]) for n, (src, mid, dst) in enumerate(moves)]
    for get in gets:
        get.start()
    for get, put in zip(gets, puts):
        get.wait()
        put.start()
    for put in puts:
        put.wait()


def local_attn(queries, key_seq, value_seq, out_grad):
    any_spec = pl.BlockSpec(memory_space=pl.ANY)
    o_x, dq_x, dkv_x = pl.pallas_call(
        attn_kernel,
        out_shape=(
            jax.ShapeDtypeStruct((N_SEQ, 2, ROWS, HEAD), BF16),
            jax.ShapeDtypeStruct((N_SEQ, 2, ROWS, HEAD), BF16),
            jax.ShapeDtypeStruct((2, N_SEQ, SHARD, HEAD), BF16),
        ),
        in_specs=[any_spec] * 4,
        out_specs=[any_spec] * 3,
        scratch_shapes=[
            pltpu.VMEM((N_DEV, SHARD, 2, HEAD), BF16),
            pltpu.VMEM((N_DEV, SHARD, 2, HEAD), BF16),
            pltpu.VMEM((2, N_DEV, SHARD, HEAD), BF16),
            pltpu.VMEM((N_DEV, HEAD, ROWS), BF16),
            pltpu.VMEM((N_DEV, HEAD, ROWS), BF16),
            pltpu.VMEM((N_DEV, HEAD, SHARD), BF16),
            pltpu.VMEM((N_DEV, HEAD, ROWS), F32),
            pltpu.VMEM((2, N_DEV, HEAD, SHARD), F32),
            pltpu.VMEM((N_DEV, ROWS, HEAD), BF16),
            pltpu.VMEM((N_DEV, HEAD, SHARD), F32),
            pltpu.VMEM((2, SUB, SHARD), BF16),
            pltpu.VMEM((2, SUB, SHARD), BF16),
            pltpu.VMEM((2, SHARD, SUB), F32),
            pltpu.VMEM((N_DEV, 1, ROWS), F32),
            pltpu.VMEM((N_DEV, 1, ROWS), F32),
            pltpu.SemaphoreType.DMA((4, N_DEV)),
            pltpu.SemaphoreType.DMA((4, N_DEV)),
            pltpu.SemaphoreType.DMA((N_DEV,)),
            pltpu.SemaphoreType.DMA((N_DEV,)),
            pltpu.SemaphoreType.DMA((4, N_DEV)),
            pltpu.SemaphoreType.DMA((4, N_DEV)),
            pltpu.SemaphoreType.DMA((7,)),
        ],
        compiler_params=pltpu.CompilerParams(
            collective_id=0, has_side_effects=True, vmem_limit_bytes=67043328),
        name='ctx_attn',
    )(queries.reshape(N_SEQ, SHARD, 2, 2, HEAD), key_seq.reshape(N_SEQ, SHARD, HEAD),
      value_seq.reshape(N_SEQ, SHARD, HEAD), out_grad.reshape(N_SEQ, SHARD, 2, 2, HEAD))
    rows_shape = jax.ShapeDtypeStruct((N_SEQ, SHARD, 2, 2, HEAD), BF16)
    keys_shape = jax.ShapeDtypeStruct((N_SEQ, SHARD, HEAD), BF16)
    attn_out, q_grad, k_grad, v_grad = pl.pallas_call(
        join_kernel,
        out_shape=(rows_shape, rows_shape, keys_shape, keys_shape),
        in_specs=[any_spec] * 3,
        out_specs=[any_spec] * 4,
        scratch_shapes=[
            pltpu.VMEM((2, N_SEQ, 2, SHARD, 2, HEAD), BF16),
            pltpu.VMEM((2, N_SEQ, SHARD, HEAD), BF16),
            pltpu.SemaphoreType.DMA((18,)),
            pltpu.SemaphoreType.DMA((18,)),
        ],
        name='join_heads',
    )(o_x.reshape(N_SEQ, 2, SHARD, 2, HEAD), dq_x.reshape(N_SEQ, 2, SHARD, 2, HEAD), dkv_x)
    return (attn_out.reshape(queries.shape), q_grad.reshape(queries.shape),
            k_grad.reshape(key_seq.shape), v_grad.reshape(value_seq.shape))


def solution(mesh):
    seq_spec = P('dp', ('cpo', 'cp'), None, None)
    return jax.shard_map(local_attn, mesh=mesh, in_specs=(seq_spec,) * 4, out_specs=(seq_spec,) * 4, check_vma=False)
```

```python
import functools
import math

import jax
import jax.numpy as jnp
from jax import lax
from jax.experimental import pallas as pl
from jax.experimental.pallas import tpu as pltpu
from jax.sharding import PartitionSpec as P

F32 = jnp.float32
BF16 = jnp.bfloat16
N_DEV = 8
N_SEQ = 4
SHARD = 1024
HEAD = 128
ROWS = 2 * SHARD
SUB = 512
N_SUB = ROWS // SUB
SCALE = HEAD ** -0.5
LOG2_SCALE = SCALE * math.log2(math.e)
NN = (((1,), (0,)), ((), ()))
MESH_ID = pl.DeviceIdType.MESH


def dot(lhs, rhs, dims):
    return lax.dot_general(lhs, rhs, dims, preferred_element_type=F32)


def causal(scores, key_start, token_start, fill):
    key_pos = key_start + lax.broadcasted_iota(jnp.int32, scores.shape, 0)
    row_tok = token_start + lax.broadcasted_iota(jnp.int32, scores.shape, 1) // 2
    return jnp.where(key_pos <= row_tok, scores, fill)


def attn_kernel(q_in, k_in, v_in, do_in, o_out, dq_out, dkv_out,
                q_land, do_land, kv_buf, q_t, do_t, kv_t, acc_t, dkv_t, stage, part, p_rows, ds_rows, s_buf, row_m, row_l,
                in_send, in_recv, fwd_send, fwd_recv, out_send, out_recv, loc_sem):
    y_pos = lax.axis_index('cpo')
    b_pos = lax.axis_index('cp')
    x_pos = b_pos // 2
    core = b_pos % 2
    chip = y_pos * 2 + x_pos
    me = chip * 2 + core
    mate = chip * 2 + 1 - core

    def dev(shard):
        return (lax.axis_index('dp'), shard // 4, shard % 4)

    def chip_at(rel):
        return ((y_pos + rel // 2) % 2) * 2 + (x_pos + rel % 2) % 2

    def by_code(code):
        return chip_at(code // 2) * 2 + (core + code % 2) % 2

    def arrival(n):
        u = n // 2
        near = (u * (3 - u)) // 2
        late = n // 4 - n // 6
        far = n // 6
        bit = (core + n % 2) % 2
        rel = near * ((1 - late) * (1 + bit) + late * (2 - bit)) + 3 * far
        return chip_at(rel) * 2 + (1 - far) * bit + far * (n % 2)

    def departure(n):
        u = n // 2
        mid = (u * (3 - u)) // 2
        rel = 3 * ((3 - u) // 3) + mid * (1 + n % 2)
        cidx = (1 - mid) * (n % 2) + mid * (u - 1)
        return chip_at(rel) * 2 + cidx

    kv_in = (k_in, v_in)

    def kv_copy(what, to, source):
        return pltpu.make_async_remote_copy(
            src_ref=kv_in[what].at[to // 2], dst_ref=kv_buf.at[what, source],
            send_sem=in_send.at[what, to], recv_sem=in_recv.at[what, source], device_id=dev(to), device_id_type=MESH_ID)

    def kv_direct(source):
        return pltpu.make_async_remote_copy(
            src_ref=k_in.at[0], dst_ref=kv_buf.at[core, source],
            send_sem=in_send.at[core, source], recv_sem=in_recv.at[core, source], device_id=dev(mate), device_id_type=MESH_ID)

    def kv_pass(source, what):
        return pltpu.make_async_remote_copy(
            src_ref=kv_buf.at[what, source], dst_ref=kv_buf.at[what, source],
            send_sem=fwd_send.at[source], recv_sem=fwd_recv.at[source], device_id=dev(mate), device_id_type=MESH_ID)

    def row_copy(what, to, source):
        src, dst = (q_in, q_land) if what == 2 else (do_in, do_land)
        return pltpu.make_async_remote_copy(
            src_ref=src.at[to // 2, :, to % 2], dst_ref=dst.at[source],
            send_sem=in_send.at[what, to], recv_sem=in_recv.at[what, source], device_id=dev(to), device_id_type=MESH_ID)

    def own_copy(what):
        if what < 2:
            return pltpu.make_async_copy(kv_in[what].at[chip], kv_buf.at[what, me], loc_sem.at[what])
        src, dst = (q_in, q_land) if what == 2 else (do_in, do_land)
        return pltpu.make_async_copy(src.at[chip, :, core], dst.at[me], loc_sem.at[what])

    barrier = pltpu.get_barrier_semaphore()
    for code in range(1, N_DEV):
        pl.semaphore_signal(barrier, inc=1, device_id=dev(by_code(code)), device_id_type=MESH_ID)
    for what in range(4):
        own_copy(what).start()
    pl.semaphore_wait(barrier, N_DEV - 1)

    for what in range(2):
        kv_copy(what, mate, me).start()
    row_copy(2, mate, me).start()
    def send_kv(rel):
        for what in range(2):
            kv_copy(what, chip_at(rel) * 2 + what, me).start()

    def send_q(rel):
        for flip in range(2):
            row_copy(2, chip_at(rel) * 2 + (core + flip) % 2, me).start()

    def send_kvq(rel):
        send_kv(rel)
        send_q(rel)

    def send_do():
        row_copy(3, mate, me).start()
        for rel in (3, 1 + core):
            for flip in range(2):
                row_copy(3, chip_at(rel) * 2 + (core + flip) % 2, me).start()
        row_copy(3, chip_at(2 - core) * 2 + 1 - core, me).start()

    send_kv(1 + core)

    def turn(land, dst, shard):
        for c in range(N_SUB):
            blk = land[shard, pl.ds(c * SUB // 2, SUB // 2)].reshape(SUB, HEAD)
            dst[shard, :, pl.ds(c * SUB, SUB)] = blk.T

    def fwd_diag(i):
        part_keys = SUB // 2

        def scores(c):
            rows = pl.ds(c * SUB, SUB)
            last = dot(kv_buf[0, i, pl.ds(c * part_keys, part_keys), :], q_t[i, :, rows], NN)
            if c == 0:
                return None, last
            return dot(kv_buf[0, i, pl.ds(0, c * part_keys), :], q_t[i, :, rows], NN), last

        here = scores(0)
        for c in range(N_SUB):
            following = scores(c + 1) if c + 1 < N_SUB else None
            rows = pl.ds(c * SUB, SUB)
            first, last = here
            last = causal(last, 0, 0, -jnp.inf)
            mx = jnp.max(last, axis=0, keepdims=True)
            if first is not None:
                mx = jnp.maximum(mx, jnp.max(first, axis=0, keepdims=True))
            p_t = jnp.exp2((last - mx) * LOG2_SCALE)
            total = jnp.sum(p_t, axis=0, keepdims=True)
            out = dot(kv_t[i, :, pl.ds(c * part_keys, part_keys)], p_t.astype(BF16), NN)
            if first is not None:
                p_t = jnp.exp2((first - mx) * LOG2_SCALE)
                total += jnp.sum(p_t, axis=0, keepdims=True)
                out += dot(kv_t[i, :, pl.ds(0, c * part_keys)], p_t.astype(BF16), NN)
            row_m[i, :, rows] = mx
            row_l[i, :, rows] = total
            acc_t[i, :, rows] = out
            here = following

    def pass_on(shard):
        kv_direct(shard).wait_recv()
        kv_pass(shard, core).start()

    def beside_last(n):
        @pl.when(n == 2)
        def _():
            send_kv(2 - core)
            row_copy(3, chip_at(2 - core) * 2 + core, me).start()

        @pl.when(n == 3)
        def _():
            pass_on(arrival(4))
            pass_on(arrival(5))
            send_q(2 - core)

    def fwd_pairs(new, n):
        def pair_of(t):
            old = arrival(t)
            return jnp.maximum(new, old), jnp.minimum(new, old)

        def scores(i, j, c):
            return dot(kv_buf[0, j], q_t[i, :, pl.ds(c * SUB, SUB)], NN)

        def softmax(i, j, c):
            rows = pl.ds(c * SUB, SUB)
            s_t = s_buf[c % 2]
            old = row_m[i, :, rows]
            mx = jnp.maximum(old, jnp.max(s_t, axis=0, keepdims=True))
            keep = jnp.exp2((old - mx) * LOG2_SCALE)
            row_m[i, :, rows] = mx
            total, out = row_l[i, :, rows] * keep, acc_t[i, :, rows] * keep
            for k0 in range(0, SHARD, SHARD // 2):
                p_t = jnp.exp2((s_t[k0:k0 + SHARD // 2] - mx) * LOG2_SCALE)
                total += jnp.sum(p_t, axis=0, keepdims=True)
                out += dot(kv_t[j, :, pl.ds(k0, SHARD // 2)], p_t.astype(BF16), NN)
            row_l[i, :, rows] = total
            acc_t[i, :, rows] = out

        def pair(t, carry):
            @pl.when(t == n - 1)
            def _():
                beside_last(n)

            i, j = pair_of(t)
            i_next, j_next = pair_of(jnp.minimum(t + 1, n - 1))
            for c in range(N_SUB):
                s_buf[(c + 1) % 2] = scores(i, j, c + 1) if c + 1 < N_SUB else scores(i_next, j_next, 0)
                softmax(i, j, c)
            return carry

        @pl.when(n > 0)
        def _():
            s_buf[0] = scores(*pair_of(0), 0)
            lax.fori_loop(0, n, pair, 0)

    def fwd_loop(n, carry):
        new = arrival(n)

        @pl.when(n == 0)
        def _():
            for what in range(3):
                own_copy(what).wait()

        @pl.when(n == 1)
        def _():
            for what in range(2):
                kv_copy(what, mate, new).wait_recv()

        @pl.when(n > 0)
        def _():
            row_copy(2, mate, new).wait_recv()

        turn(q_land, q_t, new)

        @pl.when(n > 1)
        def _():
            kv_pass(new, 1 - core).wait_recv()

        kv_t[new] = kv_buf[1, new].T
        fwd_diag(new)

        @pl.when(n == 4 + 4 * core)
        def _():
            send_kvq(3)

        @pl.when(n == 5)
        def _():
            pass_on(arrival(6))

            @pl.when(core == 1)
            def _():
                send_kvq(3)

        @pl.when(n == 6)
        def _():
            pass_on(arrival(7))
            send_do()

        fwd_pairs(new, n)

        @pl.when(n == 0)
        def _():
            pass_on(arrival(2))
            pass_on(arrival(3))
            send_q(1 + core)

        return carry
    lax.fori_loop(0, N_DEV, fwd_loop, 0)
    for n in range(2, N_DEV):
        kv_pass(arrival(n), core).wait_send()

    def out_refs(what, shard):
        if what == 2:
            return kv_buf.at[0, shard], dkv_out.at[core, chip]
        return stage.at[shard], (o_out, dq_out)[what].at[chip, core]

    def out_copy(what, shard, source):
        src, dst = out_refs(what, shard)
        return pltpu.make_async_remote_copy(
            src_ref=src, dst_ref=dst, send_sem=out_send.at[what, shard], recv_sem=out_recv.at[what, source],
            device_id=dev(shard), device_id_type=MESH_ID)

    def out_own(what):
        src, dst = out_refs(what, me)
        return pltpu.make_async_copy(src, dst, loc_sem.at[4 + what])

    def start_out(what, shard):
        @pl.when(shard == me)
        def _():
            out_own(what).start()

        @pl.when(shard != me)
        def _():
            out_copy(what, shard, me).start()

    def wait_out(what, shard):
        @pl.when(shard == me)
        def _():
            out_own(what).wait()

        @pl.when(shard != me)
        def _():
            out_copy(what, shard, me).wait_send()

    def finish_fwd(shard):
        @pl.when(shard == me)
        def _():
            own_copy(3).wait()

        @pl.when(shard != me)
        def _():
            row_copy(3, mate, shard).wait_recv()

        turn(do_land, do_t, shard)
        kv_t[shard] = kv_buf[0, shard].T
        for c in range(N_SUB):
            rows = pl.ds(c * SUB, SUB)
            total = row_l[shard, :, rows]
            o_c = (acc_t[shard, :, rows] * (1.0 / total)).astype(BF16)
            stage[shard, rows, :] = o_c.T
            row_m[shard, :, rows] = row_m[shard, :, rows] * LOG2_SCALE + jnp.log2(total)
            row_l[shard, :, rows] = jnp.sum(o_c.astype(F32) * do_t[shard, :, rows].astype(F32), axis=0, keepdims=True)
            acc_t[shard, :, rows] = jnp.zeros((HEAD, SUB), F32)
        dkv_t[0, shard] = jnp.zeros((HEAD, SHARD), F32)
        dkv_t[1, shard] = jnp.zeros((HEAD, SHARD), F32)
        start_out(0, shard)

    def bwd_block(i, row0, j, nkeys, token0, slot):
        keys = pl.ds(0, nkeys)
        rows = pl.ds(row0, SUB)
        s_t = dot(kv_buf[0, j, keys, :], q_t[i, :, rows], NN)
        dp_t = dot(kv_buf[1, j, keys, :], do_t[i, :, rows], NN)
        p_t = jnp.exp2(s_t * LOG2_SCALE - row_m[i, :, rows])
        if token0 is not None:
            p_t = causal(p_t, 0, token0, 0.0)
        ds_t = (p_t * (dp_t - row_l[i, :, rows])).astype(BF16)
        p_rows[slot, :, keys] = p_t.astype(BF16).T
        ds_rows[slot, :, keys] = ds_t.T
        acc_t[i, :, rows] += dot(kv_t[j, :, keys], ds_t, NN)
        dkv_t[0, j, :, keys] += dot(do_t[i, :, rows], p_rows[slot, :, keys], NN)
        dkv_t[1, j, :, keys] += dot(q_t[i, :, rows], ds_rows[slot, :, keys], NN)

    def bwd_diag(i):
        for c in range(N_SUB):
            bwd_block(i, c * SUB, i, (c + 1) * (SUB // 2), c * (SUB // 2), c % 2)

    def bwd_full(i, j):
        for c in range(N_SUB):
            bwd_block(i, c * SUB, j, SHARD, None, c % 2)

    def part_copy(shard):
        return pltpu.make_async_remote_copy(
            src_ref=dkv_t.at[1 - core, shard], dst_ref=part.at[shard], send_sem=out_send.at[3, shard],
            recv_sem=out_recv.at[3, shard], device_id=dev(mate), device_id_type=MESH_ID)

    def finish_dkv(shard):
        part_copy(shard).wait_recv()
        factor = jnp.where(core == 0, 1.0, SCALE).astype(F32)
        kv_buf[0, shard] = ((dkv_t[core, shard] + part[shard]) * factor).astype(BF16).T
        start_out(2, shard)

    finish_fwd(departure(0))

    def bwd_loop(n, carry):
        shard = departure(n)
        bwd_diag(shard)

        @pl.when(n > 4)
        def _():
            finish_dkv(departure(n - 1))

        def pair(back, carry):
            t = N_DEV + n - back
            u = t // 2
            first = 1 - (n + 7) // 8
            other = departure(t + first * core * ((u * (3 - u)) // 2) * (1 - 2 * (t % 2)))

            @pl.when(n == 0)
            def _():
                finish_fwd(other)

            bwd_full(jnp.maximum(shard, other), jnp.minimum(shard, other))
            return carry
        lax.fori_loop(n + 1, N_DEV, pair, 0)
        part_copy(shard).start()
        wait_out(0, shard)
        for c in range(N_SUB):
            rows = pl.ds(c * SUB, SUB)
            stage[shard, rows, :] = (acc_t[shard, :, rows] * SCALE).astype(BF16).T
        start_out(1, shard)

        @pl.when((n > 0) & (n < 5))
        def _():
            finish_dkv(departure(n - 1))
        return carry
    lax.fori_loop(0, N_DEV, bwd_loop, 0)
    finish_dkv(departure(N_DEV - 1))

    for what in range(2):
        kv_copy(what, mate, me).wait_send()
        for rel in (1, 2, 3):
            kv_copy(what, chip_at(rel) * 2 + what, me).wait_send()
    for code in range(1, N_DEV):
        for what in (2, 3):
            row_copy(what, by_code(code), me).wait_send()
    for n in range(N_DEV):
        shard = departure(n)
        part_copy(shard).wait_send()
        wait_out(1, shard)
        wait_out(2, shard)
    for code in range(1, N_DEV):
        source = by_code(code)
        for what in range(3):
            out_copy(what, source, source).wait_recv()


def join_kernel(o_in, dq_in, dkv_in, o_out, dq_out, dk_out, dv_out, rows, keys, get_sem, put_sem):
    moves = []
    for which, (src, dst) in enumerate(((o_in, o_out), (dq_in, dq_out))):
        for seq in range(N_SEQ):
            for pair in range(2):
                moves.append((src.at[seq, pair], rows.at[which, seq, pair], dst.at[seq, :, pair]))
    for which, dst in enumerate((dv_out, dk_out)):
        moves.append((dkv_in.at[which], keys.at[which], dst))
    gets = [pltpu.make_async_copy(src, mid, get_sem.at[n]) for n, (src, mid, dst) in enumerate(moves)]
    puts = [pltpu.make_async_copy(mid, dst, put_sem.at[n]) for n, (src, mid, dst) in enumerate(moves)]
    for get in gets:
        get.start()
    for get, put in zip(gets, puts):
        get.wait()
        put.start()
    for put in puts:
        put.wait()


def local_attn(queries, key_seq, value_seq, out_grad):
    any_spec = pl.BlockSpec(memory_space=pl.ANY)
    o_x, dq_x, dkv_x = pl.pallas_call(
        attn_kernel,
        out_shape=(
            jax.ShapeDtypeStruct((N_SEQ, 2, ROWS, HEAD), BF16),
            jax.ShapeDtypeStruct((N_SEQ, 2, ROWS, HEAD), BF16),
            jax.ShapeDtypeStruct((2, N_SEQ, SHARD, HEAD), BF16),
        ),
        in_specs=[any_spec] * 4,
        out_specs=[any_spec] * 3,
        scratch_shapes=[
            pltpu.VMEM((N_DEV, SHARD, 2, HEAD), BF16),
            pltpu.VMEM((N_DEV, SHARD, 2, HEAD), BF16),
            pltpu.VMEM((2, N_DEV, SHARD, HEAD), BF16),
            pltpu.VMEM((N_DEV, HEAD, ROWS), BF16),
            pltpu.VMEM((N_DEV, HEAD, ROWS), BF16),
            pltpu.VMEM((N_DEV, HEAD, SHARD), BF16),
            pltpu.VMEM((N_DEV, HEAD, ROWS), F32),
            pltpu.VMEM((2, N_DEV, HEAD, SHARD), F32),
            pltpu.VMEM((N_DEV, ROWS, HEAD), BF16),
            pltpu.VMEM((N_DEV, HEAD, SHARD), F32),
            pltpu.VMEM((2, SUB, SHARD), BF16),
            pltpu.VMEM((2, SUB, SHARD), BF16),
            pltpu.VMEM((2, SHARD, SUB), F32),
            pltpu.VMEM((N_DEV, 1, ROWS), F32),
            pltpu.VMEM((N_DEV, 1, ROWS), F32),
            pltpu.SemaphoreType.DMA((4, N_DEV)),
            pltpu.SemaphoreType.DMA((4, N_DEV)),
            pltpu.SemaphoreType.DMA((N_DEV,)),
            pltpu.SemaphoreType.DMA((N_DEV,)),
            pltpu.SemaphoreType.DMA((4, N_DEV)),
            pltpu.SemaphoreType.DMA((4, N_DEV)),
            pltpu.SemaphoreType.DMA((7,)),
        ],
        compiler_params=pltpu.CompilerParams(
            collective_id=0, has_side_effects=True, vmem_limit_bytes=67043328),
        name='ctx_attn',
    )(queries.reshape(N_SEQ, SHARD, 2, 2, HEAD), key_seq.reshape(N_SEQ, SHARD, HEAD),
      value_seq.reshape(N_SEQ, SHARD, HEAD), out_grad.reshape(N_SEQ, SHARD, 2, 2, HEAD))
    rows_shape = jax.ShapeDtypeStruct((N_SEQ, SHARD, 2, 2, HEAD), BF16)
    keys_shape = jax.ShapeDtypeStruct((N_SEQ, SHARD, HEAD), BF16)
    attn_out, q_grad, k_grad, v_grad = pl.pallas_call(
        join_kernel,
        out_shape=(rows_shape, rows_shape, keys_shape, keys_shape),
        in_specs=[any_spec] * 3,
        out_specs=[any_spec] * 4,
        scratch_shapes=[
            pltpu.VMEM((2, N_SEQ, 2, SHARD, 2, HEAD), BF16),
            pltpu.VMEM((2, N_SEQ, SHARD, HEAD), BF16),
            pltpu.SemaphoreType.DMA((18,)),
            pltpu.SemaphoreType.DMA((18,)),
        ],
        name='join_heads',
    )(o_x.reshape(N_SEQ, 2, SHARD, 2, HEAD), dq_x.reshape(N_SEQ, 2, SHARD, 2, HEAD), dkv_x)
    return (attn_out.reshape(queries.shape), q_grad.reshape(queries.shape),
            k_grad.reshape(key_seq.shape), v_grad.reshape(value_seq.shape))


def solution(mesh):
    seq_spec = P('dp', ('cpo', 'cp'), None, None)
    return jax.shard_map(local_attn, mesh=mesh, in_specs=(seq_spec,) * 4, out_specs=(seq_spec,) * 4, check_vma=False)
```
